32 devices in a mesh: grp: 8 (over y, x, core), col: 4 (over z).
Axes of the slice: x: 2, y: 2, z: 4, core: 2. Of those that a mesh axis runs over, the one named last changes fastest.
Arguments:
- old_tables: bfloat16 [32, 128, 32768], P(('grp', 'col')), may hold values from -3 to 3
- table_rows: int32 [32], replicated, may hold values from 4096 to 32768, as said below
- old_plan: int32 [32], replicated, may hold values from 0 to 31, each once
- new_plan: int32 [32], replicated, may hold values from 0 to 31, each once
- ids: int32 [256, 32, 16], P(('grp', 'col')), may hold values from 0 to 32767, as said below
- bag_len: int32 [256, 32], P(('grp', 'col')), may hold values from 1 to 16
Outputs:
- new_tables: bfloat16 [32, 128, 32768], P('grp', 'col')
- pooled: float32 [256, 32, 128], P(('grp', 'col'))
The draws below stay inside these ranges and needn't reach their ends.
Inputs may be any that keep to these rules, and one draw needn't show every extreme that they name: table_rows[t] is a multiple of 4096, and some table has exactly 32768 rows. `ids`: every id of table t lies below table_rows[t].
All inputs are finite; a program needn't handle non-finite values.
Results may differ from the reference program's by a relative error of at most 0.001.
Values may be sent and summed in bfloat16 or wider, within the bound.
A program may use at most 128 MiB of HBM per device.

```python
import jax
import jax.numpy as jnp
from jax import lax

W = 128
ROWS = 32768
BAG = 16
TABLES = 32
BATCH = 256


def table_sizes(key):
    base = jax.random.fold_in(key, 7)
    eighths = jax.random.randint(jax.random.fold_in(base, 1), (TABLES,), 1, 9)
    chosen = jax.random.randint(jax.random.fold_in(base, 2), (), 0, TABLES)
    eighths = jnp.where(jnp.arange(TABLES) == chosen, 8, eighths)
    return (eighths * (ROWS // 8)).astype(jnp.int32)


def draw_table_rows(key, part):
    return table_sizes(key)


def draw_ids(key, part):
    limits = table_sizes(key)
    drawn = jax.random.randint(jax.random.fold_in(key, 11), (BATCH, TABLES, BAG), 0, limits[None, :, None])
    return drawn.astype(jnp.int32)


def with_ends(values, own_key, low, largest):
    longest = values.shape.index(max(values.shape))
    spots = []
    for shift in (0, 1):
        where = [jax.random.randint(jax.random.fold_in(own_key, axis), (), 0, length) for axis, length in enumerate(values.shape)]
        where[longest] = (where[longest] + shift) % values.shape[longest]
        spots.append(tuple(where))
    return values.at[spots[0]].set(low).at[spots[1]].set(largest)


def shard_levels(key, dims, shards, smallest, largest):
    def one(dim, parts):
        heights = jax.random.uniform(jax.random.fold_in(jax.random.fold_in(key, 6), dim), (parts,), jnp.float32, smallest / len(shards), largest / len(shards))
        return jnp.repeat(jnp.exp(heights), dims[dim] // parts).reshape((-1,) + (1,) * (len(dims) - dim - 1))

    loudness = one(*shards[0])
    for cut in shards[1:]:
        loudness = loudness * one(*cut)
    return loudness


def centred(stream_key, shape, spread, bound, cuts=(), held_as=jnp.bfloat16):
    result = jax.random.normal(stream_key, shape, jnp.float32) * spread
    if len(cuts) > 0:
        result = shard_levels(stream_key, shape, cuts, -0.22, 0.18) * result
    return jnp.clip(result, min=-bound, max=bound).astype(held_as)


def setup_inputs(seed: int = 0) -> dict:
    splits = jax.random.split(jax.random.key(seed), 7)
    return {
        "old_tables": centred(splits[0], (TABLES, W, ROWS), 0.5, 3.0, ((0, 32),)),
        "table_rows": draw_table_rows(jax.random.fold_in(splits[6], 71), 0),
        "old_plan": jax.random.permutation(splits[2], TABLES).astype(jnp.int32),
        "new_plan": jax.random.permutation(splits[3], TABLES).astype(jnp.int32),
        "ids": draw_ids(jax.random.fold_in(splits[6], 71), 0),
        "bag_len": with_ends(jax.random.randint(splits[5], (BATCH, TABLES), 1, BAG + 1), jax.random.fold_in(splits[5], 1), 1, BAG).astype(jnp.int32),
    }


def reference(old_tables, table_rows, old_plan, new_plan, ids, bag_len):
    old_inverse = jnp.argsort(old_plan).astype(jnp.int32)
    new_inverse = jnp.argsort(new_plan).astype(jnp.int32)
    row_iota = jnp.arange(ROWS, dtype=jnp.int32)
    bag_iota = jnp.arange(BAG, dtype=jnp.int32)

    def one_table(position):
        table_id = new_plan[position]
        old_slot = old_inverse[table_id]
        stored = lax.dynamic_index_in_dim(old_tables, old_slot, 0, keepdims=False)
        keep_rows = (row_iota < table_rows[table_id]).astype(old_tables.dtype)
        masked = stored * keep_rows[None, :]
        table_ids = lax.dynamic_index_in_dim(ids, table_id, 1, keepdims=False)
        lengths = lax.dynamic_index_in_dim(bag_len, table_id, 1, keepdims=False)
        values = jnp.take(masked, table_ids, axis=1).astype(jnp.float32)
        in_bag = (bag_iota[None, :] < lengths[:, None]).astype(jnp.float32)
        sums = jnp.sum(values * in_bag[None, :, :], axis=2)
        return masked, sums

    new_tables, sums = lax.map(one_table, jnp.arange(TABLES, dtype=jnp.int32))
    pooled = jnp.transpose(sums[new_inverse], (2, 0, 1))
    return new_tables, pooled
```

```python
import functools

import jax
import jax.numpy as jnp
from jax import lax
from jax.experimental import pallas as pl
from jax.experimental.pallas import tpu as pltpu
from jax.sharding import PartitionSpec as P

MESH = pl.DeviceIdType.MESH


def invert(permutation):
    entries = permutation.shape[0]
    across = lax.broadcasted_iota(jnp.int32, (entries, entries), 1)
    down = lax.broadcasted_iota(jnp.int32, (entries, entries), 0)
    return jnp.sum(jnp.where(permutation[None, :] == down, across, 0), axis=1)


def pool_rows(table_cols, marked):
    columns = table_cols.shape[0]
    safe_ids = jnp.maximum(marked, 0).reshape(-1)
    weights = (marked >= 0).astype(jnp.float32)
    picked = (
        jnp.take(table_cols, safe_ids, axis=1)
        .reshape(columns, marked.shape[0], marked.shape[1])
        .astype(jnp.float32)
    )
    return jnp.sum(picked * weights[None, :, :], axis=2)


def move_kernel(groups, cols, chunks, source_ref, table_ref, out_ref, *scratch):
    zbufs, spreads, picks = scratch[:chunks], scratch[chunks : 2 * chunks], scratch[2 * chunks : 3 * chunks]
    z_send, z_recv, s_send, s_recv, p_send, p_recv = scratch[3 * chunks :]
    g = lax.axis_index("grp")
    c = lax.axis_index("col")
    per_group, narrow, table_len = out_ref.shape
    chunk_rows = table_len // chunks
    sub = chunk_rows // groups

    def aligned(value, unit):
        return pl.multiple_of(value * unit, unit)

    def column_step(k, d):
        to = lax.rem(c + d, cols)
        src = table_ref.at[0, pl.ds(aligned(to, narrow), narrow), pl.ds(k * chunk_rows, chunk_rows)]
        dst = zbufs[k].at[c]
        if d == 0:
            return pltpu.make_async_copy(src, dst, z_recv.at[k, d])
        return pltpu.make_async_remote_copy(
            src, dst, z_send.at[k, d], z_recv.at[k, d], device_id=(g, to), device_id_type=MESH
        )

    def spread_step(k, d):
        to = lax.rem(g + d, groups)
        src = zbufs[k].at[:, :, pl.ds(aligned(to, sub), sub)]
        dst = spreads[k].at[pl.ds(g * cols, cols)]
        if d == 0:
            return pltpu.make_async_copy(src, dst, s_recv.at[k, d])
        return pltpu.make_async_remote_copy(
            src, dst, s_send.at[k, d], s_recv.at[k, d], device_id=(to, c), device_id_type=MESH
        )

    def group_step(k, d):
        to = lax.rem(g + d, groups)
        src = picks[k].at[pl.ds(to * per_group, per_group)]
        dst = out_ref.at[:, :, pl.ds(aligned(k * groups + g, sub), sub)]
        if d == 0:
            return pltpu.make_async_copy(src, dst, p_recv.at[k, d])
        return pltpu.make_async_remote_copy(
            src, dst, p_send.at[k, d], p_recv.at[k, d], device_id=(to, c), device_id_type=MESH
        )

    def finish(copy, d):
        if d == 0:
            copy.wait()
        else:
            copy.wait_recv()

    col_order = [d for d in (2, 1, 3) if d < cols] + list(range(4, cols)) + [0]
    grp_order = list(range(1, groups)) + [0]

    for k in range(chunks):
        for d in col_order:
            column_step(k, d).start()

    def route(k):
        for d in grp_order:
            finish(spread_step(k, d), d)

        def pick(i, carry):
            picks[k][i] = spreads[k][source_ref[i]]
            return carry

        lax.fori_loop(0, groups * per_group, pick, 0)
        for d in grp_order:
            group_step(k, d).start()

    for k in range(chunks):
        for d in col_order:
            finish(column_step(k, d), d)
        for d in grp_order:
            spread_step(k, d).start()
        if k > 0:
            route(k - 1)
    route(chunks - 1)
    for k in range(chunks):
        for d in grp_order:
            finish(group_step(k, d), d)
        for d in col_order:
            if d > 0:
                column_step(k, d).wait_send()
        for d in grp_order:
            if d > 0:
                spread_step(k, d).wait_send()
                group_step(k, d).wait_send()


def move_tables(old_tables, source_slot, groups, cols):
    _, width, table_len = old_tables.shape
    narrow = width // cols
    tables = source_slot.shape[0]
    per_group = tables // groups
    chunks = min(8, table_len // (groups * 128))
    chunk_rows = table_len // chunks
    sub = chunk_rows // groups
    dtype = old_tables.dtype
    sems = [
        pltpu.SemaphoreType.DMA((chunks, n)) for n in (cols, cols, groups, groups, groups, groups)
    ]
    return pl.pallas_call(
        functools.partial(move_kernel, groups, cols, chunks),
        out_shape=jax.ShapeDtypeStruct((per_group, narrow, table_len), dtype),
        in_specs=[
            pl.BlockSpec(memory_space=pltpu.SMEM),
            pl.BlockSpec(memory_space=pl.ANY),
        ],
        out_specs=pl.BlockSpec(memory_space=pl.ANY),
        scratch_shapes=[pltpu.VMEM((cols, narrow, chunk_rows), dtype)] * chunks
        + [pltpu.VMEM((groups * cols, narrow, sub), dtype)] * chunks
        + [pltpu.VMEM((tables, narrow, sub), dtype)] * chunks
        + sems,
        compiler_params=pltpu.CompilerParams(
            has_side_effects=True, vmem_limit_bytes=48 * 1024 * 1024
        ),
    )(source_slot, old_tables)


def body(old_tables, table_rows, old_plan, new_plan, ids, bag_len):
    group_count = lax.axis_size("grp")
    col_count = lax.axis_size("col")
    full_width = old_tables.shape[1]
    table_len = old_tables.shape[2]
    per_group = new_plan.shape[0] // group_count
    bag_size = ids.shape[2]
    old_inverse = invert(old_plan)
    moved = move_tables(old_tables, old_inverse[new_plan], group_count, col_count)
    new_ids = lax.dynamic_slice_in_dim(new_plan, lax.axis_index("grp") * per_group, per_group)
    limits = table_rows[new_ids]
    row_iota = lax.broadcasted_iota(jnp.int32, (1, 1, table_len), 2)
    new_local = jnp.where(row_iota < limits[:, None, None], moved, jnp.zeros((), moved.dtype))
    bag_iota = lax.broadcasted_iota(jnp.int32, (1, 1, bag_size), 2)
    marked = jnp.where(bag_iota < bag_len[:, :, None], ids, -1)
    by_slot = jnp.take(marked, old_plan, axis=1)
    own_ids = lax.all_to_all(
        by_slot, ("grp", "col"), split_axis=1, concat_axis=0, tiled=True
    ).reshape(-1, bag_size)
    partial_value = pool_rows(old_tables[0], own_ids)
    returned = lax.all_to_all(
        partial_value.reshape(1, full_width, -1),
        ("grp", "col"),
        split_axis=2,
        concat_axis=0,
        tiled=True,
    )
    by_table = jnp.take(returned, old_inverse, axis=0)
    pooled = jnp.transpose(by_table, (2, 0, 1))
    return (new_local, pooled)


def solution(mesh):
    return jax.shard_map(
        body,
        mesh=mesh,
        in_specs=(
            P(("grp", "col"), None, None),
            P(),
            P(),
            P(),
            P(("grp", "col"), None, None),
            P(("grp", "col"), None),
        ),
        out_specs=(P("grp", "col", None), P(("grp", "col"), None, None)),
        check_vma=False,
    )
```

```python
import functools

import jax
import jax.numpy as jnp
from jax import lax
from jax.experimental import pallas as pl
from jax.experimental.pallas import tpu as pltpu
from jax.sharding import PartitionSpec as P

WINDOW = 2
CHUNKS = 16
MESH = pl.DeviceIdType.MESH


def invert(permutation):
    entries = permutation.shape[0]
    across = lax.broadcasted_iota(jnp.int32, (entries, entries), 1)
    down = lax.broadcasted_iota(jnp.int32, (entries, entries), 0)
    return jnp.sum(jnp.where(permutation[None, :] == down, across, 0), axis=1)


def move_kernel(groups, cols, chunks, source_ref, table_ref, ids_ref, out_ref, sums_ref, *scratch):
    zbufs, spreads, picks = scratch[:chunks], scratch[chunks : 2 * chunks], scratch[2 * chunks : 3 * chunks]
    z_send, z_recv, s_send, s_recv, p_send, p_recv = scratch[3 * chunks : 3 * chunks + 6]
    own_ids, tabs, total, i_send, i_recv, r_send, r_recv, t_sem = scratch[3 * chunks + 6 :]
    g = lax.axis_index("grp")
    c = lax.axis_index("col")
    per_group, narrow, table_len = out_ref.shape
    chunk_rows = table_len // chunks
    sub = chunk_rows // groups

    def aligned(value, unit):
        return pl.multiple_of(value * unit, unit)

    def column_step(k, d):
        to = lax.rem(c + d, cols)
        src = table_ref.at[0, pl.ds(aligned(to, narrow), narrow), pl.ds(k * chunk_rows, chunk_rows)]
        dst = zbufs[k].at[c]
        if d == 0:
            return pltpu.make_async_copy(src, dst, z_recv.at[k, d])
        return pltpu.make_async_remote_copy(
            src, dst, z_send.at[k, d], z_recv.at[k, d], device_id=(g, to), device_id_type=MESH
        )

    def spread_step(k, d):
        to = lax.rem(g + d, groups)
        src = zbufs[k].at[:, :, pl.ds(aligned(to, sub), sub)]
        dst = spreads[k].at[pl.ds(g * cols, cols)]
        if d == 0:
            return pltpu.make_async_copy(src, dst, s_recv.at[k, d])
        return pltpu.make_async_remote_copy(
            src, dst, s_send.at[k, d], s_recv.at[k, d], device_id=(to, c), device_id_type=MESH
        )

    def group_step(k, d):
        to = lax.rem(g + d, groups)
        src = picks[k].at[pl.ds(to * per_group, per_group)]
        dst = out_ref.at[:, :, pl.ds(aligned(k * groups + g, sub), sub)]
        if d == 0:
            return pltpu.make_async_copy(src, dst, p_recv.at[k, d])
        return pltpu.make_async_remote_copy(
            src, dst, p_send.at[k, d], p_recv.at[k, d], device_id=(to, c), device_id_type=MESH
        )

    devices = groups * cols
    me = g * cols + c
    samples, bag = ids_ref.shape[1:]

    def ids_step(d):
        to = lax.rem(me + d, devices)
        src, dst = ids_ref.at[to], own_ids.at[me]
        if isinstance(d, int):
            return pltpu.make_async_copy(src, dst, i_recv.at[d])
        return pltpu.make_async_remote_copy(
            src, dst, i_send.at[d], i_recv.at[d],
            device_id=(to // cols, lax.rem(to, cols)), device_id_type=MESH,
        )

    def sums_step(d):
        to = lax.rem(me + d, devices)
        src, dst = total.at[to], sums_ref.at[me]
        if isinstance(d, int):
            return pltpu.make_async_copy(src, dst, r_recv.at[d])
        return pltpu.make_async_remote_copy(
            src, dst, r_send.at[d], r_recv.at[d],
            device_id=(to // cols, lax.rem(to, cols)), device_id_type=MESH,
        )

    def each_peer(act):
        def step(d, carry):
            act(d)
            return carry

        lax.fori_loop(1, devices, step, 0)

    def fetch(k):
        return pltpu.make_async_copy(
            table_ref.at[0, :, pl.ds(k * chunk_rows, chunk_rows)], tabs.at[k % 2], t_sem.at[k % 2]
        )

    tile = 512 if chunk_rows % 512 == 0 else 128
    fold = 8 if devices % 8 == 0 else 1

    def pool(k):
        fetch(k).wait()
        if k + 1 < chunks:
            fetch(k + 1).start()
        columns = chunk_rows // tile

        def piece(step, carry):
            block, part = step // columns, lax.rem(step, columns)
            rows = samples * fold
            wanted = own_ids[pl.ds(block * fold, fold)].reshape(rows, bag)
            row = lax.broadcasted_iota(jnp.int32, (rows, tile), 1) + (k * chunk_rows + part * tile)
            counts = jnp.zeros((rows, tile), jnp.float32)
            for i in range(bag):
                counts = jnp.where(wanted[:, i : i + 1] == row, counts + 1.0, counts)
            values = tabs[k % 2, :, pl.ds(aligned(part, tile), tile)]
            sums = lax.dot_general(
                counts.astype(values.dtype), values, (((1,), (1,)), ((), ())),
                preferred_element_type=jnp.float32,
            )
            where = pl.ds(block * fold, fold)
            total[where] = total[where] + sums.reshape(fold, samples, values.shape[0])
            return carry

        lax.fori_loop(0, devices // fold * columns, piece, 0)

    def finish(copy, d):
        if d == 0:
            copy.wait()
        else:
            copy.wait_recv()

    col_order = [d for d in (2, 1, 3) if d < cols] + list(range(4, cols)) + [0]
    grp_order = list(range(1, groups)) + [0]

    each_peer(lambda d: ids_step(d).start())
    ids_step(0).start()
    fetch(0).start()
    for k in range(min(WINDOW, chunks)):
        for d in col_order:
            column_step(k, d).start()
    total[...] = jnp.zeros_like(total)
    each_peer(lambda d: ids_step(d).wait_recv())
    ids_step(0).wait()

    def route(k):
        for d in grp_order:
            finish(spread_step(k, d), d)

        def pick(i, carry):
            picks[k][i] = spreads[k][source_ref[i]]
            return carry

        lax.fori_loop(0, groups * per_group, pick, 0)
        for d in grp_order:
            group_step(k, d).start()

    for k in range(chunks):
        for d in col_order:
            finish(column_step(k, d), d)
        for d in grp_order:
            spread_step(k, d).start()
        if k + WINDOW < chunks:
            for d in col_order:
                column_step(k + WINDOW, d).start()
        if k > 0:
            route(k - 1)
        pool(k)
    each_peer(lambda d: sums_step(d).start())
    sums_step(0).start()
    route(chunks - 1)
    for k in range(chunks):
        for d in grp_order:
            finish(group_step(k, d), d)
        for d in col_order:
            if d > 0:
                column_step(k, d).wait_send()
        for d in grp_order:
            if d > 0:
                spread_step(k, d).wait_send()
                group_step(k, d).wait_send()
    each_peer(lambda d: ids_step(d).wait_send())
    each_peer(lambda d: sums_step(d).wait())
    sums_step(0).wait()


def move_tables(old_tables, source_slot, by_slot, groups, cols):
    _, width, table_len = old_tables.shape
    narrow = width // cols
    tables = source_slot.shape[0]
    per_group = tables // groups
    chunks = min(CHUNKS, table_len // (groups * 128))
    chunk_rows = table_len // chunks
    sub = chunk_rows // groups
    dtype = old_tables.dtype
    devices, samples, _ = by_slot.shape
    sems = [
        pltpu.SemaphoreType.DMA((chunks, n)) for n in (cols, cols, groups, groups, groups, groups)
    ]
    return pl.pallas_call(
        functools.partial(move_kernel, groups, cols, chunks),
        out_shape=(
            jax.ShapeDtypeStruct((per_group, narrow, table_len), dtype),
            jax.ShapeDtypeStruct((devices, samples, width), jnp.float32),
        ),
        in_specs=[
            pl.BlockSpec(memory_space=pltpu.SMEM),
            pl.BlockSpec(memory_space=pl.ANY),
            pl.BlockSpec(memory_space=pltpu.VMEM),
        ],
        out_specs=(pl.BlockSpec(memory_space=pl.ANY), pl.BlockSpec(memory_space=pltpu.VMEM)),
        scratch_shapes=[pltpu.VMEM((cols, narrow, chunk_rows), dtype)] * chunks
        + [pltpu.VMEM((groups * cols, narrow, sub), dtype)] * chunks
        + [pltpu.VMEM((tables, narrow, sub), dtype)] * chunks
        + sems
        + [
            pltpu.VMEM(by_slot.shape, by_slot.dtype),
            pltpu.VMEM((2, width, chunk_rows), dtype),
            pltpu.VMEM((devices, samples, width), jnp.float32),
        ]
        + [pltpu.SemaphoreType.DMA((devices,))] * 4
        + [pltpu.SemaphoreType.DMA((2,))],
        compiler_params=pltpu.CompilerParams(
            has_side_effects=True, vmem_limit_bytes=48 * 1024 * 1024
        ),
    )(source_slot, old_tables, by_slot)


def body(old_tables, table_rows, old_plan, new_plan, ids, bag_len):
    group_count = lax.axis_size("grp")
    col_count = lax.axis_size("col")
    table_len = old_tables.shape[2]
    per_group = new_plan.shape[0] // group_count
    bag_size = ids.shape[2]
    old_inverse = invert(old_plan)
    bag_iota = lax.broadcasted_iota(jnp.int32, (1, 1, bag_size), 2)
    marked = jnp.where(bag_iota < bag_len[:, :, None], ids, -1)
    by_slot = jnp.transpose(jnp.take(marked, old_plan, axis=1), (1, 0, 2))
    moved, sums = move_tables(old_tables, old_inverse[new_plan], by_slot, group_count, col_count)
    new_ids = lax.dynamic_slice_in_dim(new_plan, lax.axis_index("grp") * per_group, per_group)
    limits = table_rows[new_ids]
    row_iota = lax.broadcasted_iota(jnp.int32, (1, 1, table_len), 2)
    new_local = jnp.where(row_iota < limits[:, None, None], moved, jnp.zeros((), moved.dtype))
    pooled = jnp.transpose(jnp.take(sums, old_inverse, axis=0), (1, 0, 2))
    return (new_local, pooled)


def solution(mesh):
    return jax.shard_map(
        body,
        mesh=mesh,
        in_specs=(
            P(("grp", "col"), None, None),
            P(),
            P(),
            P(),
            P(("grp", "col"), None, None),
            P(("grp", "col"), None),
        ),
        out_specs=(P("grp", "col", None), P(("grp", "col"), None, None)),
        check_vma=False,
    )
```

```python
import functools

import jax
import jax.numpy as jnp
from jax import lax
from jax.experimental import pallas as pl
from jax.experimental.pallas import tpu as pltpu
from jax.sharding import PartitionSpec as P

WINDOW = 2
CHUNKS = 32
ORDER = (4, 2, 6, 3, 5, 7, 1)
MESH = pl.DeviceIdType.MESH


def move_kernel(groups, cols, chunks, old_ref, new_ref, table_ref, ids_ref, out_ref, pooled_ref, *scratch):
    zbufs, spreads, picks = scratch[:chunks], scratch[chunks : 2 * chunks], scratch[2 * chunks : 3 * chunks]
    z_send, z_recv, s_send, s_recv, p_send, p_recv = scratch[3 * chunks : 3 * chunks + 6]
    own_ids, by_slot, tabs, total, sums_ref, source_ref, inverse_ref = scratch[3 * chunks + 6 : 3 * chunks + 13]
    i_send, i_recv, r_send, r_recv, t_sem = scratch[3 * chunks + 13 :]
    g = lax.axis_index("grp")
    c = lax.axis_index("col")
    per_group, narrow, table_len = out_ref.shape
    chunk_rows = table_len // chunks
    sub = chunk_rows // groups

    def aligned(value, unit):
        return pl.multiple_of(value * unit, unit)

    def column_step(k, d):
        to = lax.rem(c + d, cols)
        src = table_ref.at[0, pl.ds(aligned(to, narrow), narrow), pl.ds(k * chunk_rows, chunk_rows)]
        dst = zbufs[k].at[c]
        if d == 0:
            return pltpu.make_async_copy(src, dst, z_recv.at[k, d])
        return pltpu.make_async_remote_copy(
            src, dst, z_send.at[k, d], z_recv.at[k, d], device_id=(g, to), device_id_type=MESH
        )

    def spread_step(k, d):
        to = lax.rem(g + d, groups)
        src = zbufs[k].at[:, :, pl.ds(aligned(to, sub), sub)]
        dst = spreads[k].at[pl.ds(g * cols, cols)]
        if d == 0:
            return pltpu.make_async_copy(src, dst, s_recv.at[k, d])
        return pltpu.make_async_remote_copy(
            src, dst, s_send.at[k, d], s_recv.at[k, d], device_id=(to, c), device_id_type=MESH
        )

    def group_step(k, d):
        to = lax.rem(g + d, groups)
        src = picks[k].at[pl.ds(to * per_group, per_group)]
        dst = out_ref.at[:, :, pl.ds(aligned(k * groups + g, sub), sub)]
        if d == 0:
            return pltpu.make_async_copy(src, dst, p_recv.at[k, d])
        return pltpu.make_async_remote_copy(
            src, dst, p_send.at[k, d], p_recv.at[k, d], device_id=(to, c), device_id_type=MESH
        )

    devices = groups * cols
    me = g * cols + c
    samples, tables, bag = ids_ref.shape

    def ids_step(d):
        to = lax.rem(me + d, devices)
        src, dst = by_slot.at[to], own_ids.at[me]
        if isinstance(d, int):
            return pltpu.make_async_copy(src, dst, i_recv.at[d])
        return pltpu.make_async_remote_copy(
            src, dst, i_send.at[d], i_recv.at[d],
            device_id=(to // cols, lax.rem(to, cols)), device_id_type=MESH,
        )

    def sums_step(d):
        to = lax.rem(me + d, devices)
        src, dst = total.at[to], sums_ref.at[me]
        if isinstance(d, int):
            return pltpu.make_async_copy(src, dst, r_recv.at[d])
        return pltpu.make_async_remote_copy(
            src, dst, r_send.at[d], r_recv.at[d],
            device_id=(to // cols, lax.rem(to, cols)), device_id_type=MESH,
        )

    def each_peer(act):
        def step(d, carry):
            act(d)
            return carry

        lax.fori_loop(1, devices, step, 0)

    def fetch(k):
        return pltpu.make_async_copy(
            table_ref.at[0, :, pl.ds(k * chunk_rows, chunk_rows)], tabs.at[k % 2], t_sem.at[k % 2]
        )

    tile = 512 if chunk_rows % 512 == 0 else 128
    fold = 8 if devices % 8 == 0 else 1

    def pool(k):
        fetch(k).wait()
        if k + 1 < chunks:
            fetch(k + 1).start()
        columns = chunk_rows // tile

        def piece(step, carry):
            block, part = step // columns, lax.rem(step, columns)
            rows = samples * fold
            wanted = own_ids[pl.ds(block * fold, fold)].reshape(rows, bag)
            row = lax.broadcasted_iota(jnp.int32, (rows, tile), 1) + (k * chunk_rows + part * tile)
            counts = jnp.zeros((rows, tile), jnp.float32)
            for i in range(bag):
                counts = jnp.where(wanted[:, i : i + 1] == row, counts + 1.0, counts)
            values = tabs[k % 2, :, pl.ds(aligned(part, tile), tile)]
            sums = lax.dot_general(
                counts.astype(values.dtype), values, (((1,), (1,)), ((), ())),
                preferred_element_type=jnp.float32,
            )
            where = pl.ds(block * fold, fold)
            total[where] = total[where] + sums.reshape(fold, samples, values.shape[0])
            return carry

        lax.fori_loop(0, devices // fold * columns, piece, 0)

    def finish(copy, d):
        if d == 0:
            copy.wait()
        else:
            copy.wait_recv()

    col_order = [d for d in (2, 1, 3) if d < cols] + list(range(4, cols)) + [0]
    grp_order = [d for d in ORDER if d < groups] + list(range(8, groups)) + [0]

    def order_ids(s, carry):
        by_slot[s] = ids_ref[:, pl.ds(old_ref[s], 1), :].reshape(samples, bag)
        return carry

    def locate(j, carry):
        wanted = new_ref[j]

        def look(s, found):
            held = old_ref[s]
            return jnp.where(held == wanted, s, found[0]), jnp.where(held == j, s, found[1])

        source_ref[j], inverse_ref[j] = lax.fori_loop(0, tables, look, (0, 0))
        return carry

    for k in range(min(WINDOW, chunks)):
        for d in col_order:
            column_step(k, d).start()
    fetch(0).start()
    lax.fori_loop(0, tables, order_ids, 0)
    lax.fori_loop(0, tables, locate, 0)
    each_peer(lambda d: ids_step(d).start())
    ids_step(0).start()
    total[...] = jnp.zeros_like(total)
    each_peer(lambda d: ids_step(d).wait_recv())
    ids_step(0).wait()

    def route(k):
        for d in grp_order:
            finish(spread_step(k, d), d)

        def pick(i, carry):
            picks[k][i] = spreads[k][source_ref[i]]
            return carry

        lax.fori_loop(0, groups * per_group, pick, 0)
        for d in grp_order:
            group_step(k, d).start()

    for k in range(chunks):
        for d in col_order:
            finish(column_step(k, d), d)
        for d in grp_order:
            spread_step(k, d).start()
        if k + WINDOW < chunks:
            for d in col_order:
                column_step(k + WINDOW, d).start()
        if k > 0:
            route(k - 1)
        pool(k)
    route(chunks - 1)
    each_peer(lambda d: sums_step(d).start())
    sums_step(0).start()
    for k in range(chunks):
        for d in grp_order:
            finish(group_step(k, d), d)
        for d in col_order:
            if d > 0:
                column_step(k, d).wait_send()
        for d in grp_order:
            if d > 0:
                spread_step(k, d).wait_send()
                group_step(k, d).wait_send()
    each_peer(lambda d: ids_step(d).wait_send())
    each_peer(lambda d: sums_step(d).wait())
    sums_step(0).wait()
    for t in range(tables):
        pooled_ref[:, t, :] = sums_ref[inverse_ref[t]]


def move_tables(old_tables, old_plan, new_plan, marked, groups, cols):
    _, width, table_len = old_tables.shape
    narrow = width // cols
    tables = old_plan.shape[0]
    per_group = tables // groups
    chunks = min(CHUNKS, table_len // (groups * 128))
    chunk_rows = table_len // chunks
    sub = chunk_rows // groups
    dtype = old_tables.dtype
    devices = groups * cols
    samples, _, bag = marked.shape
    sems = [
        pltpu.SemaphoreType.DMA((chunks, n)) for n in (cols, cols, groups, groups, groups, groups)
    ]
    return pl.pallas_call(
        functools.partial(move_kernel, groups, cols, chunks),
        out_shape=(
            jax.ShapeDtypeStruct((per_group, narrow, table_len), dtype),
            jax.ShapeDtypeStruct((samples, tables, width), jnp.float32),
        ),
        in_specs=[
            pl.BlockSpec(memory_space=pltpu.SMEM),
            pl.BlockSpec(memory_space=pltpu.SMEM),
            pl.BlockSpec(memory_space=pl.ANY),
            pl.BlockSpec(memory_space=pltpu.VMEM),
        ],
        out_specs=(pl.BlockSpec(memory_space=pl.ANY), pl.BlockSpec(memory_space=pltpu.VMEM)),
        scratch_shapes=[pltpu.VMEM((cols, narrow, chunk_rows), dtype)] * chunks
        + [pltpu.VMEM((groups * cols, narrow, sub), dtype)] * chunks
        + [pltpu.VMEM((tables, narrow, sub), dtype)] * chunks
        + sems
        + [
            pltpu.VMEM((devices, samples, bag), marked.dtype),
            pltpu.VMEM((devices, samples, bag), marked.dtype),
            pltpu.VMEM((2, width, chunk_rows), dtype),
            pltpu.VMEM((devices, samples, width), jnp.float32),
            pltpu.VMEM((devices, samples, width), jnp.float32),
            pltpu.SMEM((tables,), jnp.int32),
            pltpu.SMEM((tables,), jnp.int32),
        ]
        + [pltpu.SemaphoreType.DMA((devices,))] * 4
        + [pltpu.SemaphoreType.DMA((2,))],
        compiler_params=pltpu.CompilerParams(
            has_side_effects=True, vmem_limit_bytes=48 * 1024 * 1024
        ),
    )(old_plan, new_plan, old_tables, marked)


def clear_kernel(per_group, step, plan_ref, rows_ref, moved_ref, out_ref):
    own = lax.axis_index("grp") * per_group + pl.program_id(0)
    limit = rows_ref[plan_ref[own]] - pl.program_id(1) * step
    row = lax.broadcasted_iota(jnp.int32, moved_ref.shape, 2)
    out_ref[...] = jnp.where(row < limit, moved_ref[...], jnp.zeros_like(moved_ref))


def clear_unused(moved, new_plan, table_rows):
    per_group, narrow, table_len = moved.shape
    step = min(8192, table_len)

    def source(p, r, plan_ref, rows_ref):
        own = lax.axis_index("grp") * per_group + p
        return p, 0, jnp.minimum(r, (rows_ref[plan_ref[own]] - 1) // step)

    return pl.pallas_call(
        functools.partial(clear_kernel, per_group, step),
        out_shape=jax.ShapeDtypeStruct(moved.shape, moved.dtype),
        grid_spec=pltpu.PrefetchScalarGridSpec(
            num_scalar_prefetch=2,
            grid=(per_group, table_len // step),
            in_specs=[pl.BlockSpec((1, narrow, step), source)],
            out_specs=pl.BlockSpec((1, narrow, step), lambda p, r, *_: (p, 0, r)),
        ),
    )(new_plan, table_rows, moved)


def body(old_tables, table_rows, old_plan, new_plan, ids, bag_len):
    group_count = lax.axis_size("grp")
    col_count = lax.axis_size("col")
    bag_iota = lax.broadcasted_iota(jnp.int32, (1, 1, ids.shape[2]), 2)
    marked = jnp.where(bag_iota < bag_len[:, :, None], ids, -1)
    moved, pooled = move_tables(old_tables, old_plan, new_plan, marked, group_count, col_count)
    return (clear_unused(moved, new_plan, table_rows), pooled)


def solution(mesh):
    return jax.shard_map(
        body,
        mesh=mesh,
        in_specs=(
            P(("grp", "col"), None, None),
            P(),
            P(),
            P(),
            P(("grp", "col"), None, None),
            P(("grp", "col"), None),
        ),
        out_specs=(P("grp", "col", None), P(("grp", "col"), None, None)),
        check_vma=False,
    )
```

```python
import functools

import jax
import jax.numpy as jnp
from jax import lax
from jax.experimental import pallas as pl
from jax.experimental.pallas import tpu as pltpu
from jax.sharding import PartitionSpec as P

WINDOW = 2
CHUNKS = 32
ORDER = (4, 2, 6, 3, 5, 7, 1)
MESH = pl.DeviceIdType.MESH


def move_kernel(groups, cols, chunks, old_ref, new_ref, table_ref, ids_ref, out_ref, pooled_ref, *scratch):
    zbufs, spreads, picks = scratch[:chunks], scratch[chunks : 2 * chunks], scratch[2 * chunks : 3 * chunks]
    z_send, z_recv, s_send, s_recv, p_send, p_recv = scratch[3 * chunks : 3 * chunks + 6]
    own_ids, by_slot, tabs, total, sums_ref, source_ref, inverse_ref = scratch[3 * chunks + 6 : 3 * chunks + 13]
    i_send, i_recv, r_send, r_recv, t_sem = scratch[3 * chunks + 13 :]
    g = lax.axis_index("grp")
    c = lax.axis_index("col")
    per_group, narrow, table_len = out_ref.shape
    chunk_rows = table_len // chunks
    sub = chunk_rows // groups

    def aligned(value, unit):
        return pl.multiple_of(value * unit, unit)

    def column_step(k, d):
        to = lax.rem(c + d, cols)
        src = table_ref.at[0, pl.ds(aligned(to, narrow), narrow), pl.ds(k * chunk_rows, chunk_rows)]
        dst = zbufs[k].at[c]
        if d == 0:
            return pltpu.make_async_copy(src, dst, z_recv.at[k, d])
        return pltpu.make_async_remote_copy(
            src, dst, z_send.at[k, d], z_recv.at[k, d], device_id=(g, to), device_id_type=MESH
        )

    def spread_step(k, d):
        to = lax.rem(g + d, groups)
        src = zbufs[k].at[:, :, pl.ds(aligned(to, sub), sub)]
        dst = spreads[k].at[pl.ds(g * cols, cols)]
        if d == 0:
            return pltpu.make_async_copy(src, dst, s_recv.at[k, d])
        return pltpu.make_async_remote_copy(
            src, dst, s_send.at[k, d], s_recv.at[k, d], device_id=(to, c), device_id_type=MESH
        )

    def group_step(k, d):
        to = lax.rem(g + d, groups)
        src = picks[k].at[pl.ds(to * per_group, per_group)]
        dst = out_ref.at[:, :, pl.ds(aligned(k * groups + g, sub), sub)]
        if d == 0:
            return pltpu.make_async_copy(src, dst, p_recv.at[k, d])
        return pltpu.make_async_remote_copy(
            src, dst, p_send.at[k, d], p_recv.at[k, d], device_id=(to, c), device_id_type=MESH
        )

    devices = groups * cols
    me = g * cols + c
    samples, tables, bag = ids_ref.shape

    def ids_step(d):
        to = lax.rem(me + d, devices)
        src, dst = by_slot.at[to], own_ids.at[me]
        if isinstance(d, int):
            return pltpu.make_async_copy(src, dst, i_recv.at[d])
        return pltpu.make_async_remote_copy(
            src, dst, i_send.at[d], i_recv.at[d],
            device_id=(to // cols, lax.rem(to, cols)), device_id_type=MESH,
        )

    def sums_step(d):
        to = lax.rem(me + d, devices)
        src, dst = total.at[to], sums_ref.at[me]
        if isinstance(d, int):
            return pltpu.make_async_copy(src, dst, r_recv.at[d])
        return pltpu.make_async_remote_copy(
            src, dst, r_send.at[d], r_recv.at[d],
            device_id=(to // cols, lax.rem(to, cols)), device_id_type=MESH,
        )

    def each_peer(act):
        def step(d, carry):
            act(d)
            return carry

        lax.fori_loop(1, devices, step, 0)

    def fetch(k):
        return pltpu.make_async_copy(
            table_ref.at[0, :, pl.ds(k * chunk_rows, chunk_rows)], tabs.at[k % 2], t_sem.at[k % 2]
        )

    tile = 512 if chunk_rows % 512 == 0 else 128
    fold = 8 if devices % 8 == 0 else 1

    def pool(k):
        fetch(k).wait()
        if k + 1 < chunks:
            fetch(k + 1).start()
        columns = chunk_rows // tile

        def piece(step, carry):
            block, part = step // columns, lax.rem(step, columns)
            rows = samples * fold
            wanted = own_ids[pl.ds(block * fold, fold)].reshape(rows, bag)
            row = lax.broadcasted_iota(jnp.int32, (rows, tile), 1) + (k * chunk_rows + part * tile)
            counts = jnp.zeros((rows, tile), jnp.float32)
            for i in range(bag):
                counts = jnp.where(wanted[:, i : i + 1] == row, counts + 1.0, counts)
            values = tabs[k % 2, :, pl.ds(aligned(part, tile), tile)]
            sums = lax.dot_general(
                counts.astype(values.dtype), values, (((1,), (1,)), ((), ())),
                preferred_element_type=jnp.float32,
            )
            where = pl.ds(block * fold, fold)
            total[where] = total[where] + sums.reshape(fold, samples, values.shape[0])
            return carry

        lax.fori_loop(0, devices // fold * columns, piece, 0)

    def finish(copy, d):
        if d == 0:
            copy.wait()
        else:
            copy.wait_recv()

    col_order = [d for d in (2, 1, 3) if d < cols] + list(range(4, cols)) + [0]
    grp_order = [d for d in ORDER if d < groups] + list(range(8, groups)) + [0]

    def order_ids(s, carry):
        by_slot[s] = ids_ref[:, pl.ds(old_ref[s], 1), :].reshape(samples, bag)
        return carry

    def locate(j, carry):
        wanted = new_ref[j]

        source, inverse = jnp.int32(0), jnp.int32(0)
        for s in range(1, tables):
            held = old_ref[s]
            source = jnp.where(held == wanted, s, source)
            inverse = jnp.where(held == j, s, inverse)
        source_ref[j] = source
        inverse_ref[j] = inverse
        return carry

    for k in range(min(WINDOW, chunks)):
        for d in col_order:
            column_step(k, d).start()
    fetch(0).start()
    lax.fori_loop(0, tables, order_ids, 0)
    lax.fori_loop(0, tables, locate, 0)
    each_peer(lambda d: ids_step(d).start())
    ids_step(0).start()
    total[...] = jnp.zeros_like(total)

    def route(k):
        for d in grp_order:
            finish(spread_step(k, d), d)

        def pick(i, carry):
            picks[k][i] = spreads[k][source_ref[i]]
            return carry

        lax.fori_loop(0, groups * per_group, pick, 0)
        for d in grp_order:
            group_step(k, d).start()

    for k in range(chunks):
        for d in col_order:
            finish(column_step(k, d), d)
        for d in grp_order:
            spread_step(k, d).start()
        if k + WINDOW < chunks:
            for d in col_order:
                column_step(k + WINDOW, d).start()
        if k > 0:
            route(k - 1)
        if k == 0:
            each_peer(lambda d: ids_step(d).wait_recv())
            ids_step(0).wait()
            pool(0)
        if k + 1 < chunks:
            pool(k + 1)
    each_peer(lambda d: sums_step(d).start())
    sums_step(0).start()
    route(chunks - 1)
    for k in range(chunks):
        for d in grp_order:
            finish(group_step(k, d), d)
        for d in col_order:
            if d > 0:
                column_step(k, d).wait_send()
        for d in grp_order:
            if d > 0:
                spread_step(k, d).wait_send()
                group_step(k, d).wait_send()
    each_peer(lambda d: ids_step(d).wait_send())
    each_peer(lambda d: sums_step(d).wait())
    sums_step(0).wait()
    for t in range(tables):
        pooled_ref[:, t, :] = sums_ref[inverse_ref[t]]


def move_tables(old_tables, old_plan, new_plan, marked, groups, cols):
    _, width, table_len = old_tables.shape
    narrow = width // cols
    tables = old_plan.shape[0]
    per_group = tables // groups
    chunks = min(CHUNKS, table_len // (groups * 128))
    chunk_rows = table_len // chunks
    sub = chunk_rows // groups
    dtype = old_tables.dtype
    devices = groups * cols
    samples, _, bag = marked.shape
    sems = [
        pltpu.SemaphoreType.DMA((chunks, n)) for n in (cols, cols, groups, groups, groups, groups)
    ]
    return pl.pallas_call(
        functools.partial(move_kernel, groups, cols, chunks),
        out_shape=(
            jax.ShapeDtypeStruct((per_group, narrow, table_len), dtype),
            jax.ShapeDtypeStruct((samples, tables, width), jnp.float32),
        ),
        in_specs=[
            pl.BlockSpec(memory_space=pltpu.SMEM),
            pl.BlockSpec(memory_space=pltpu.SMEM),
            pl.BlockSpec(memory_space=pl.ANY),
            pl.BlockSpec(memory_space=pltpu.VMEM),
        ],
        out_specs=(pl.BlockSpec(memory_space=pl.ANY), pl.BlockSpec(memory_space=pltpu.VMEM)),
        scratch_shapes=[pltpu.VMEM((cols, narrow, chunk_rows), dtype)] * chunks
        + [pltpu.VMEM((groups * cols, narrow, sub), dtype)] * chunks
        + [pltpu.VMEM((tables, narrow, sub), dtype)] * chunks
        + sems
        + [
            pltpu.VMEM((devices, samples, bag), marked.dtype),
            pltpu.VMEM((devices, samples, bag), marked.dtype),
            pltpu.VMEM((2, width, chunk_rows), dtype),
            pltpu.VMEM((devices, samples, width), jnp.float32),
            pltpu.VMEM((devices, samples, width), jnp.float32),
            pltpu.SMEM((tables,), jnp.int32),
            pltpu.SMEM((tables,), jnp.int32),
        ]
        + [pltpu.SemaphoreType.DMA((devices,))] * 4
        + [pltpu.SemaphoreType.DMA((2,))],
        compiler_params=pltpu.CompilerParams(
            has_side_effects=True, vmem_limit_bytes=48 * 1024 * 1024
        ),
    )(old_plan, new_plan, old_tables, marked)


def body(old_tables, table_rows, old_plan, new_plan, ids, bag_len):
    group_count = lax.axis_size("grp")
    col_count = lax.axis_size("col")
    bag_iota = lax.broadcasted_iota(jnp.int32, (1, 1, ids.shape[2]), 2)
    marked = jnp.where(bag_iota < bag_len[:, :, None], ids, -1)
    moved, pooled = move_tables(old_tables, old_plan, new_plan, marked, group_count, col_count)
    per_group = moved.shape[0]
    own = lax.dynamic_slice_in_dim(new_plan, lax.axis_index("grp") * per_group, per_group)
    row = lax.broadcasted_iota(jnp.int32, (1, 1, moved.shape[2]), 2)
    used = row < table_rows[own][:, None, None]
    return (jnp.where(used, moved, jnp.zeros((), moved.dtype)), pooled)


def solution(mesh):
    return jax.shard_map(
        body,
        mesh=mesh,
        in_specs=(
            P(("grp", "col"), None, None),
            P(),
            P(),
            P(),
            P(("grp", "col"), None, None),
            P(("grp", "col"), None),
        ),
        out_specs=(P("grp", "col", None), P(("grp", "col"), None, None)),
        check_vma=False,
    )
```
